512 devices in a mesh: row: 16 (over z, core), col: 32 (over y, x).
Axes of the slice: x: 4, y: 8, z: 8, core: 2. Of those that a mesh axis runs over, the one named last changes fastest.
Arguments:
- points: float32 [16, 16384], P(None, ('row', 'col')), may hold values from -6 to 6
- pivots_first: int32 [128], replicated, may hold values from 0 to 16383, as said below
- pivots_second: int32 [128], replicated, may hold values from 0 to 16383, as said below
Outputs:
- panels: float32 [16384, 256], P('row')
- schur: float32 [16384, 16384], P('row', 'col')
The draws below stay inside these ranges and needn't reach their ends.
Inputs may be any that keep to these rules, and one draw needn't show every extreme that they name: `pivots_first`: 128 distinct indices, none of them among pivots_second. `pivots_second`: 128 distinct indices, none of them among pivots_first.
All inputs are finite; a program needn't handle non-finite values.
Results may differ from the reference program's by a relative error of at most 0.0003.
Values sent between devices are 32-bit elements; how exact they have to be, the bound alone decides.
A program may use at most 64 MiB of HBM per device.

```python
import jax
import jax.numpy as jnp
from jax import lax

DIM = 16
BLOCK = 128
NPTS = 16384
N_ROW = 16


def pivot_order(key):
    return jax.random.permutation(jax.random.fold_in(key, 11), NPTS)[:2 * BLOCK].astype(jnp.int32)


def draw_pivots_first(key, part):
    return pivot_order(key)[:BLOCK]


def draw_pivots_second(key, part):
    return pivot_order(key)[BLOCK:]


def steps_of(key, shape, pieces, smallest, high):
    def one(dim, shards_of):
        steps = jax.random.uniform(jax.random.fold_in(jax.random.fold_in(key, 6), dim), (shards_of,), jnp.float32, smallest / len(pieces), high / len(pieces))
        return jnp.repeat(jnp.exp(steps), shape[dim] // shards_of).reshape((-1,) + (1,) * (len(shape) - dim - 1))

    factor_of = one(*pieces[0])
    for cut in pieces[1:]:
        factor_of = factor_of * one(*cut)
    return factor_of


def scatter_about(key, shape, spread, bound, split=(), held_as=jnp.bfloat16):
    entries = spread * jax.random.normal(key, shape, jnp.float32)
    if split:
        entries = entries * steps_of(key, shape, split, -0.22, 0.18)
    return jnp.clip(entries, -bound, bound).astype(held_as)


def setup_inputs(seed: int = 0) -> dict:
    streams_of = jax.random.split(jax.random.key(seed), 4)
    return {
        "points": scatter_about(streams_of[0], (DIM, NPTS), 1.0, 6.0, ((1, 512),), jnp.float32),
        "pivots_first": draw_pivots_first(jax.random.fold_in(streams_of[3], 71), 0),
        "pivots_second": draw_pivots_second(jax.random.fold_in(streams_of[3], 71), 0),
    }


def kernel(left, left_ids, right, right_ids):
    left_sq = jnp.sum(left * left, axis=0)
    right_sq = jnp.sum(right * right, axis=0)
    inner = jnp.dot(left.T, right, precision=lax.Precision.HIGHEST)
    dist = left_sq[:, None] + right_sq[None, :] - 2.0 * inner
    same = (left_ids[:, None] == right_ids[None, :]).astype(jnp.float32)
    return jnp.exp(-dist / DIM) + 0.1 * same

def right_solve(root, columns):
    return jax.scipy.linalg.solve_triangular(root, columns.T, lower=True).T

def reference(points, pivots_first, pivots_second):
    ids = jnp.arange(NPTS, dtype=jnp.int32)
    first_pts = points[:, pivots_first]
    second_pts = points[:, pivots_second]
    first_columns = kernel(points, ids, first_pts, pivots_first)
    first_root = jnp.linalg.cholesky(first_columns[pivots_first])
    first_panel = right_solve(first_root, first_columns)
    first_pivot_rows = first_panel[pivots_second]
    second_columns = kernel(points, ids, second_pts, pivots_second) - jnp.dot(first_panel, first_pivot_rows.T, precision=lax.Precision.HIGHEST)
    second_root = jnp.linalg.cholesky(second_columns[pivots_second])
    second_panel = right_solve(second_root, second_columns)
    panels = jnp.concatenate([first_panel, second_panel], axis=1)
    rows_blk = NPTS // N_ROW
    blocks_pts = points.reshape(DIM, N_ROW, rows_blk).transpose(1, 0, 2)
    blocks_ids = ids.reshape(N_ROW, rows_blk)
    blocks_pan = panels.reshape(N_ROW, rows_blk, 2 * BLOCK)

    def one_block(item):
        blk_pts, blk_ids, blk_pan = item
        whole = kernel(blk_pts, blk_ids, points, ids)
        return whole - jnp.dot(blk_pan, panels.T, precision=lax.Precision.HIGHEST)
    schur = lax.map(one_block, (blocks_pts, blocks_ids, blocks_pan)).reshape(NPTS, NPTS)
    return (panels, schur)
```

```python
import functools
import jax
import jax.numpy as jnp
from jax import lax
from jax.sharding import PartitionSpec as P
from jax.experimental import pallas as pl
from jax.experimental.pallas import tpu as pltpu

DIM = 16
BLOCK = 128
PIV = 2 * BLOCK
LEAF = 32
bf16 = jnp.bfloat16
f32 = jnp.float32


def split3(x):
    hi = x.astype(bf16)
    r = x - hi.astype(f32)
    mid = r.astype(bf16)
    lo = (r - mid.astype(f32)).astype(bf16)
    return hi, mid, lo


def dot(a, b):
    return lax.dot_general(a, b, (((1,), (0,)), ((), ())), preferred_element_type=f32)


def features(pts, left):
    n = pts.shape[1]
    sq = jnp.sum(pts * pts, axis=0, keepdims=True) * (-1.0 / DIM)
    sh, sm, sl = split3(sq)
    if not left:
        pts = pts * (2.0 / DIM)
    h, m, l = split3(pts)
    row = lax.broadcasted_iota(jnp.int32, (DIM, n), 0)
    at = 0 if left else 3
    ext = jnp.where((row >= 3 - at) & (row < 6 - at), 1.0, 0.0).astype(f32)
    for i, part in enumerate((sh, sm, sl)):
        ext = jnp.where(row == at + i, jnp.broadcast_to(part.astype(f32), (DIM, n)), ext)
    ext = ext.astype(bf16)
    zero = jnp.zeros((DIM, n), bf16)
    parts = (h, h, m, m, h, l, ext, zero) if left else (h, m, h, m, l, h, ext, zero)
    return jnp.concatenate(parts, axis=0)


def leaf(a_ref, o):
    rows = a_ref[pl.ds(o, LEAF), :]
    half = (o // 128) * 128
    tile = rows[:, half:half + 128]
    lane = lax.broadcasted_iota(jnp.int32, (LEAF, PIV), 1)
    sub = lax.broadcasted_iota(jnp.int32, (LEAF, PIV), 0)
    inside = (lane >= o) & (lane < o + LEAF)
    r = jnp.where(inside, jnp.where(lane == sub + o, 1.0, 0.0), rows)
    w = o - half
    v = [jnp.broadcast_to(tile[:, w + m:w + m + 1], (LEAF, 128)) for m in range(LEAF)]
    G = LEAF // 8
    v = [[x[8 * g:8 * g + 8] for g in range(G)] for x in v]
    r = [[r[8 * g:8 * g + 8, 128 * h:128 * h + 128] for h in range(PIV // 128)] for g in range(G)]
    sub8 = lax.broadcasted_iota(jnp.int32, (8, 128), 0)
    ds = []

    def row_of(x, i):
        return jnp.broadcast_to(x[i:i + 1, :], (8, 128))

    for c in range(LEAF):
        g0, i0 = c // 8, c % 8
        d = row_of(v[c][g0], i0)
        ds.append(d)
        inv = 1.0 / d
        mult = {}
        for g in range(g0, G):
            x = v[c][g]
            if g == g0:
                if i0 == 7:
                    continue
                x = jnp.where(sub8 > i0, x, 0.0)
            mult[g] = x * inv
        for m in range(c + 1, LEAF):
            p = row_of(v[m][g0], i0)
            for g in mult:
                v[m][g] = v[m][g] - mult[g] * p
        for h in range(PIV // 128):
            p = row_of(r[g0][h], i0)
            for g in mult:
                r[g][h] = r[g][h] - mult[g] * p
    out = []
    for g in range(G):
        d = ds[8 * g]
        for i in range(1, 8):
            d = jnp.where(sub8 == i, ds[8 * g + i], d)
        s = lax.rsqrt(d)
        out.append(jnp.concatenate([x * s for x in r[g]], axis=1))
    return jnp.concatenate(out, axis=0)


def factor(a_ref):
    for k in range(PIV // LEAF):
        o = k * LEAF
        u = leaf(a_ref, o)
        lane = lax.broadcasted_iota(jnp.int32, (LEAF, PIV), 1)
        a_ref[pl.ds(o, LEAF), :] = jnp.where(lane < o + LEAF, u, 0.0)
        left = PIV - o - LEAF
        if left:
            h, m, l = split3(u)
            lhs = jnp.concatenate((h, h, m, m, h, l), axis=0)
            rhs = jnp.concatenate((h, m, h, m, l, h), axis=0)
            start = ((o + LEAF) // 128) * 128
            lt = lhs[:, start:].T
            lt = lt[o + LEAF - start:, :]
            upd = dot(lt, rhs)
            lane = lax.broadcasted_iota(jnp.int32, (left, PIV), 1)
            old = a_ref[pl.ds(o + LEAF, left), :]
            old = jnp.where((lane >= o) & (lane < o + LEAF), 0.0, old)
            a_ref[pl.ds(o + LEAF, left), :] = old - upd


def dot6(ls, rs):
    lh, lm, ll = ls
    rh, rm, rl = rs
    return (dot(ll, rh) + dot(lh, rl) + dot(lm, rm)) + (dot(lm, rh) + dot(lh, rm)) + dot(lh, rh)


def dot3(ls, rs):
    lh, lm = ls[:2]
    rh, rm = rs[:2]
    return (dot(lm, rh) + dot(lh, rm)) + dot(lh, rh)


def kernel_b(base_ref, pivl_ref, pivs_ref, pt_ref, rt_ref, ct_ref, panel_ref, schur_ref,
             a_ref, fr_ref, fp_ref, fc_ref, wt_ref, pc_ref, *, tile, six):
    t = pl.program_id(0)
    n_rows, n_cols = rt_ref.shape[1], ct_ref.shape[1]

    @pl.when(t == 0)
    def _():
        pt = pt_ref[...]
        fp = features(pt, False)
        fp_ref[...] = fp
        fpl = features(pt, True).T
        kpp = jnp.exp(dot(fpl, fp))
        i = lax.broadcasted_iota(jnp.int32, (PIV, PIV), 0)
        j = lax.broadcasted_iota(jnp.int32, (PIV, PIV), 1)
        a_ref[...] = jnp.where(i == j, kpp + 0.1, kpp)
        fr_ref[...] = features(rt_ref[...], True).T
        fc = features(ct_ref[...], False)
        fc_ref[...] = fc
        factor(a_ref)
        w = a_ref[...]
        kpc = jnp.exp(dot(fpl, fc))
        cid = base_ref[1] + lax.broadcasted_iota(jnp.int32, (PIV, n_cols), 1)
        kpc = kpc + jnp.where(cid == pivs_ref[...], 0.1, 0.0)
        pc = dot6(split3(w), split3(kpc))
        for q, x in enumerate(split3(pc)):
            pc_ref[q] = x
        for q, x in enumerate(split3(w.T)):
            wt_ref[q] = x

    fr = fr_ref[pl.ds(pl.multiple_of(t * tile, tile), tile), :]
    krp = jnp.exp(dot(fr, fp_ref[...]))
    rid = base_ref[0] + t * tile + lax.broadcasted_iota(jnp.int32, (tile, PIV), 0)
    krp = krp + jnp.where(rid == pivl_ref[...], 0.1, 0.0)
    panel = dot6(split3(krp), (wt_ref[0], wt_ref[1], wt_ref[2]))
    panel_ref[...] = panel
    krc = jnp.exp(dot(fr, fc_ref[...]))
    off = base_ref[1] - base_ref[0] - t * tile
    i = lax.broadcasted_iota(jnp.int32, (tile, n_cols), 0)
    j = lax.broadcasted_iota(jnp.int32, (tile, n_cols), 1)
    krc = krc + jnp.where(i == j + off, 0.1, 0.0)
    mul = dot6 if six else dot3
    schur_ref[...] = krc - mul(split3(panel), (pc_ref[0], pc_ref[1], pc_ref[2]))


def compute(base, pivots, pt, rt, ct, tile=128, six=True):
    n_rows, n_cols = rt.shape[1], ct.shape[1]
    whole = lambda x: pl.BlockSpec(x.shape, lambda t: (0,) * x.ndim)
    pivl = pivots[None, :]
    pivs = pivots[:, None]
    return pl.pallas_call(
        functools.partial(kernel_b, tile=tile, six=six),
        grid=(n_rows // tile,),
        out_shape=(
            jax.ShapeDtypeStruct((n_rows, PIV), f32),
            jax.ShapeDtypeStruct((n_rows, n_cols), f32),
        ),
        in_specs=[pl.BlockSpec(memory_space=pltpu.SMEM)] + [whole(x) for x in (pivl, pivs, pt, rt, ct)],
        out_specs=(
            pl.BlockSpec((tile, PIV), lambda t: (t, 0)),
            pl.BlockSpec((tile, n_cols), lambda t: (t, 0)),
        ),
        scratch_shapes=[
            pltpu.VMEM((PIV, PIV), f32),
            pltpu.VMEM((n_rows, 128), bf16),
            pltpu.VMEM((128, PIV), bf16),
            pltpu.VMEM((128, n_cols), bf16),
            pltpu.VMEM((3, PIV, PIV), bf16),
            pltpu.VMEM((3, PIV, n_cols), bf16),
        ],
        compiler_params=pltpu.CompilerParams(vmem_limit_bytes=48 << 20),
    )(base, pivl, pivs, pt, rt, ct)


MESH = pl.DeviceIdType.MESH


def gather_kernel(nz, ny, nx, pts_ref, own_ref, piv_ref, piv_out, row_out, col_out,
                  contrib, rs_buf, y_src, y_buf, z_src, z_buf,
                  rs_send, rs_recv, y_send, y_recv, z_send, z_recv, ag_send, ag_recv,
                  row_send, row_recv, col_send, col_recv):
    n_row, n_col = 2 * nz, ny * nx
    row = lax.axis_index("row")
    col = lax.axis_index("col")
    core, z = row % 2, row // 2
    x, y = col % nx, col // nx
    ring = 2 * nx
    me = 2 * x + core

    def ring_dev(u):
        return (2 * z + u % 2, nx * y + u // 2)

    def y_dev(d):
        return (row, nx * ((y + d) % ny) + x)

    def z_dev(d):
        return (2 * ((z + d) % nz) + core, col)

    def row_dev(d):
        return (row, (col + d) % n_col)

    wide = n_col // n_row
    per = n_col // wide
    target = wide * row + col // per
    part = col % per
    source = col // wide
    first = (col % wide) * per

    barrier = pltpu.get_barrier_semaphore()

    def signal(dev):
        pl.semaphore_signal(barrier, inc=1, device_id=dev, device_id_type=MESH)

    def loop(lo, hi, f):
        def body(i, carry):
            f(i)
            return carry
        lax.fori_loop(lo, hi, body, 0)

    loop(1, ring, lambda d: signal(ring_dev((me + d) % ring)))
    loop(1, ny, lambda d: signal(y_dev(d)))
    loop(1, nz, lambda d: signal(z_dev(d)))
    loop(1, n_col, lambda d: signal(row_dev(d)))

    self_source = jnp.logical_and(source == row, col // per == col % wide)

    def greet_source(i):
        @pl.when(jnp.logical_or(source != row, first + i != col))
        def _():
            signal((source, first + i))

    loop(0, per, greet_source)

    pts = pts_ref[...]
    n = pts.shape[1]
    mine = (row * n_col + col) * n
    hit = piv_ref[...] == mine + lax.broadcasted_iota(jnp.int32, (n, PIV), 0)
    hot = jnp.where(hit, 1.0, 0.0).astype(bf16)
    h, m, l = split3(pts)
    got = (dot(l, hot) + dot(m, hot)) + dot(h, hot)
    quarter = 4
    for u in range(8):
        half, c4 = u // 4, u % 4
        contrib[u] = got[4 * c4:4 * c4 + 4, 128 * half:128 * half + 128]
    row_out[col] = own_ref[...]

    to_me = n_row - 1 + jnp.where(target == col, 0, 1)
    pl.semaphore_wait(barrier, (ring - 1) + (ny - 1) + (nz - 1) + (n_col - 1) + to_me)

    def rs_copy(d):
        u = (me + d) % ring
        return pltpu.make_async_remote_copy(
            src_ref=contrib.at[u], dst_ref=rs_buf.at[d - 1], send_sem=rs_send.at[d - 1],
            recv_sem=rs_recv.at[d - 1], device_id=ring_dev(u), device_id_type=MESH)

    def y_copy(d):
        return pltpu.make_async_remote_copy(
            src_ref=y_src, dst_ref=y_buf.at[d - 1], send_sem=y_send.at[d - 1],
            recv_sem=y_recv.at[d - 1], device_id=y_dev(d), device_id_type=MESH)

    def z_copy(d):
        return pltpu.make_async_remote_copy(
            src_ref=z_src, dst_ref=z_buf.at[d - 1], send_sem=z_send.at[d - 1],
            recv_sem=z_recv.at[d - 1], device_id=z_dev(d), device_id_type=MESH)

    def ag_copy(d):
        return pltpu.make_async_remote_copy(
            src_ref=piv_out.at[me], dst_ref=piv_out.at[me], send_sem=ag_send.at[d - 1],
            recv_sem=ag_recv.at[d - 1], device_id=ring_dev((me + d) % ring), device_id_type=MESH)

    def row_copy(d):
        return pltpu.make_async_remote_copy(
            src_ref=own_ref, dst_ref=row_out.at[col], send_sem=row_send.at[d - 1],
            recv_sem=row_recv.at[d - 1], device_id=row_dev(d), device_id_type=MESH)

    def col_copy(d):
        return pltpu.make_async_remote_copy(
            src_ref=own_ref, dst_ref=col_out.at[part], send_sem=col_send.at[d],
            recv_sem=col_recv.at[part], device_id=((row + d) % n_row, target), device_id_type=MESH)

    def col_arrival(i):
        return pltpu.make_async_remote_copy(
            src_ref=own_ref, dst_ref=col_out.at[i], send_sem=col_send.at[0],
            recv_sem=col_recv.at[i], device_id=(row, col), device_id_type=MESH)

    for d in range(1, ring):
        rs_copy(d).start()
    loop(1, n_col, lambda d: row_copy(d).start())

    @pl.when(target != col)
    def _():
        col_copy(0).start()

    @pl.when(target == col)
    def _():
        col_out[part] = own_ref[...]

    loop(1, n_row, lambda d: col_copy(d).start())

    total = contrib[me]
    for d in range(1, ring):
        rs_copy(d).wait_recv()
        total = total + rs_buf[d - 1]
    y_src[...] = total
    for d in range(1, ny):
        y_copy(d).start()
    for d in range(1, ny):
        y_copy(d).wait_recv()
        total = total + y_buf[d - 1]
    z_src[...] = total
    for d in range(1, nz):
        z_copy(d).start()
    for d in range(1, nz):
        z_copy(d).wait_recv()
        total = total + z_buf[d - 1]
    piv_out[me] = total
    for d in range(1, ring):
        ag_copy(d).start()
    loop(1, n_col, lambda d: row_copy(d).wait_recv())

    def take(i):
        @pl.when(jnp.logical_or(source != row, first + i != col))
        def _():
            col_arrival(i).wait_recv()

    loop(0, per, take)
    for d in range(1, ring):
        ag_copy(d).wait_recv()
    for d in range(1, ring):
        rs_copy(d).wait_send()
        ag_copy(d).wait_send()
    for d in range(1, ny):
        y_copy(d).wait_send()
    for d in range(1, nz):
        z_copy(d).wait_send()
    loop(1, n_col, lambda d: row_copy(d).wait_send())

    @pl.when(target != col)
    def _():
        col_copy(0).wait_send()

    loop(1, n_row, lambda d: col_copy(d).wait_send())


def gather(points, pivots, mesh):
    n_row, n_col = mesh.shape["row"], mesh.shape["col"]
    nz, nx = n_row // 2, 4
    ny = n_col // nx
    ring = 2 * nx
    own = points.reshape(4, 128)
    dma = pltpu.SemaphoreType.DMA
    vmem = pl.BlockSpec(memory_space=pltpu.VMEM)
    piv, rows, cols = pl.pallas_call(
        functools.partial(gather_kernel, nz, ny, nx),
        out_shape=(
            jax.ShapeDtypeStruct((ring, 4, 128), f32),
            jax.ShapeDtypeStruct((n_col, 4, 128), f32),
            jax.ShapeDtypeStruct((n_row, 4, 128), f32),
        ),
        in_specs=[vmem] * 3,
        out_specs=(vmem,) * 3,
        scratch_shapes=[
            pltpu.VMEM((ring, 4, 128), f32),
            pltpu.VMEM((ring - 1, 4, 128), f32),
            pltpu.VMEM((4, 128), f32),
            pltpu.VMEM((ny - 1, 4, 128), f32),
            pltpu.VMEM((4, 128), f32),
            pltpu.VMEM((nz - 1, 4, 128), f32),
            dma((ring - 1,)), dma((ring - 1,)),
            dma((ny - 1,)), dma((ny - 1,)),
            dma((nz - 1,)), dma((nz - 1,)),
            dma((ring - 1,)), dma((ring - 1,)),
            dma((n_col - 1,)), dma((n_col - 1,)),
            dma((n_row,)), dma((n_row,)),
        ],
        compiler_params=pltpu.CompilerParams(collective_id=0, has_side_effects=True),
    )(points, own, pivots[None, :])
    pt = piv.reshape(2, DIM, 128).transpose(1, 0, 2).reshape(DIM, PIV)

    def unpack(x):
        k = x.shape[0]
        return x.reshape(k, DIM, 32).transpose(1, 0, 2).reshape(DIM, k * 32)

    return pt, unpack(rows), unpack(cols)


def solution(mesh):
    def per_device(points, pivots_first, pivots_second):
        pivots = jnp.concatenate([pivots_first, pivots_second])
        pt, rt, ct = gather(points, pivots, mesh)
        base = jnp.stack([lax.axis_index("row") * rt.shape[1], lax.axis_index("col") * ct.shape[1]])
        return compute(base.astype(jnp.int32), pivots, pt, rt, ct)

    return jax.shard_map(
        per_device,
        mesh=mesh,
        in_specs=(P(None, ("row", "col")), P(), P()),
        out_specs=(P("row", None), P("row", "col")),
        check_vma=False,
    )
```

```python
import functools
import jax
import jax.numpy as jnp
from jax import lax
from jax.sharding import PartitionSpec as P
from jax.experimental import pallas as pl
from jax.experimental.pallas import tpu as pltpu

DIM = 16
BLOCK = 128
PIV = 2 * BLOCK
LEAF = 32
bf16 = jnp.bfloat16
f32 = jnp.float32


def split3(x):
    hi = x.astype(bf16)
    r = x - hi.astype(f32)
    mid = r.astype(bf16)
    lo = (r - mid.astype(f32)).astype(bf16)
    return hi, mid, lo


def dot(a, b):
    return lax.dot_general(a, b, (((1,), (0,)), ((), ())), preferred_element_type=f32)


def features(pts, left):
    n = pts.shape[1]
    sq = jnp.sum(pts * pts, axis=0, keepdims=True) * (-1.0 / DIM)
    sh, sm, sl = split3(sq)
    if not left:
        pts = pts * (2.0 / DIM)
    h, m, l = split3(pts)
    row = lax.broadcasted_iota(jnp.int32, (DIM, n), 0)
    at = 0 if left else 3
    ext = jnp.where((row >= 3 - at) & (row < 6 - at), 1.0, 0.0).astype(f32)
    for i, part in enumerate((sh, sm, sl)):
        ext = jnp.where(row == at + i, jnp.broadcast_to(part.astype(f32), (DIM, n)), ext)
    ext = ext.astype(bf16)
    zero = jnp.zeros((DIM, n), bf16)
    parts = (h, h, m, m, h, l, ext, zero) if left else (h, m, h, m, l, h, ext, zero)
    return jnp.concatenate(parts, axis=0)


def leaf(a_ref, o):
    rows = a_ref[pl.ds(o, LEAF), :]
    half = (o // 128) * 128
    tile = rows[:, half:half + 128]
    lane = lax.broadcasted_iota(jnp.int32, (LEAF, PIV), 1)
    sub = lax.broadcasted_iota(jnp.int32, (LEAF, PIV), 0)
    inside = (lane >= o) & (lane < o + LEAF)
    r = jnp.where(inside, jnp.where(lane == sub + o, 1.0, 0.0), rows)
    w = o - half
    v = [jnp.broadcast_to(tile[:, w + m:w + m + 1], (LEAF, 128)) for m in range(LEAF)]
    G = LEAF // 8
    v = [[x[8 * g:8 * g + 8] for g in range(G)] for x in v]
    r = [[r[8 * g:8 * g + 8, 128 * h:128 * h + 128] for h in range(PIV // 128)] for g in range(G)]
    sub8 = lax.broadcasted_iota(jnp.int32, (8, 128), 0)
    ds = []

    def row_of(x, i):
        return jnp.broadcast_to(x[i:i + 1, :], (8, 128))

    for c in range(LEAF):
        g0, i0 = c // 8, c % 8
        d = row_of(v[c][g0], i0)
        ds.append(d)
        inv = 1.0 / d
        mult = {}
        for g in range(g0, G):
            x = v[c][g]
            if g == g0:
                if i0 == 7:
                    continue
                x = jnp.where(sub8 > i0, x, 0.0)
            mult[g] = x * inv
        for m in range(c + 1, LEAF):
            p = row_of(v[m][g0], i0)
            for g in mult:
                v[m][g] = v[m][g] - mult[g] * p
        for h in range(PIV // 128):
            p = row_of(r[g0][h], i0)
            for g in mult:
                r[g][h] = r[g][h] - mult[g] * p
    out = []
    for g in range(G):
        d = ds[8 * g]
        for i in range(1, 8):
            d = jnp.where(sub8 == i, ds[8 * g + i], d)
        s = lax.rsqrt(d)
        out.append(jnp.concatenate([x * s for x in r[g]], axis=1))
    return jnp.concatenate(out, axis=0)


def factor(a_ref):
    for k in range(PIV // LEAF):
        o = k * LEAF
        u = leaf(a_ref, o)
        lane = lax.broadcasted_iota(jnp.int32, (LEAF, PIV), 1)
        a_ref[pl.ds(o, LEAF), :] = jnp.where(lane < o + LEAF, u, 0.0)
        left = PIV - o - LEAF
        if left:
            h, m, l = split3(u)
            lhs = jnp.concatenate((h, h, m, m, h, l), axis=0)
            rhs = jnp.concatenate((h, m, h, m, l, h), axis=0)
            start = ((o + LEAF) // 128) * 128
            lt = lhs[:, start:].T
            lt = lt[o + LEAF - start:, :]
            upd = dot(lt, rhs)
            lane = lax.broadcasted_iota(jnp.int32, (left, PIV), 1)
            old = a_ref[pl.ds(o + LEAF, left), :]
            old = jnp.where((lane >= o) & (lane < o + LEAF), 0.0, old)
            a_ref[pl.ds(o + LEAF, left), :] = old - upd


def dot6(ls, rs):
    lh, lm, ll = ls
    rh, rm, rl = rs
    return (dot(ll, rh) + dot(lh, rl) + dot(lm, rm)) + (dot(lm, rh) + dot(lh, rm)) + dot(lh, rh)


def dot3(ls, rs):
    lh, lm = ls[:2]
    rh, rm = rs[:2]
    return (dot(lm, rh) + dot(lh, rm)) + dot(lh, rh)


def kernel_b(pid_ref, pt_ref, fr_ref, fc_ref, panel_ref, schur_ref,
             a_ref, fp_ref, wt_ref, pc_ref, *, tile):
    t = pl.program_id(0)
    n_cols = fc_ref.shape[1]
    row0 = lax.axis_index("row") * fr_ref.shape[0] + t * tile
    col0 = lax.axis_index("col") * n_cols
    piv = pid_ref[...]

    @pl.when(t == 0)
    def _():
        pt = jnp.concatenate([pt_ref[0], pt_ref[1]], axis=1)
        fp = features(pt, False)
        fp_ref[...] = fp
        fpl = features(pt, True).T
        kpp = jnp.exp(dot(fpl, fp))
        i = lax.broadcasted_iota(jnp.int32, (PIV, PIV), 0)
        j = lax.broadcasted_iota(jnp.int32, (PIV, PIV), 1)
        a_ref[...] = jnp.where(i == j, kpp + 0.1, kpp)
        kpc = jnp.exp(dot(fpl, fc_ref[...]))
        ids = jnp.broadcast_to(piv.astype(f32), (8, PIV)).T[:, 0:1].astype(jnp.int32)
        cid = col0 + lax.broadcasted_iota(jnp.int32, (PIV, n_cols), 1)
        kpc = kpc + jnp.where(cid == ids, 0.1, 0.0)
        factor(a_ref)
        w = a_ref[...]
        pc = dot6(split3(w), split3(kpc))
        for q, x in enumerate(split3(pc)):
            pc_ref[q] = x
        for q, x in enumerate(split3(w.T)):
            wt_ref[q] = x

    fr = fr_ref[pl.ds(pl.multiple_of(t * tile, tile), tile), :]
    krp = jnp.exp(dot(fr, fp_ref[...]))
    rid = row0 + lax.broadcasted_iota(jnp.int32, (tile, PIV), 0)
    krp = krp + jnp.where(rid == piv, 0.1, 0.0)
    panel = dot6(split3(krp), (wt_ref[0], wt_ref[1], wt_ref[2]))
    panel_ref[...] = panel
    krc = jnp.exp(dot(fr, fc_ref[...]))
    i = lax.broadcasted_iota(jnp.int32, (tile, n_cols), 0)
    j = lax.broadcasted_iota(jnp.int32, (tile, n_cols), 1)
    krc = krc + jnp.where(i - j == col0 - row0, 0.1, 0.0)
    schur_ref[...] = krc - dot6(split3(panel), (pc_ref[0], pc_ref[1], pc_ref[2]))


def compute(pid, pt, fr, fc, tile=256):
    n_rows, n_cols = fr.shape[0], fc.shape[1]
    vmem = pl.BlockSpec(memory_space=pltpu.VMEM)
    return pl.pallas_call(
        functools.partial(kernel_b, tile=tile),
        grid=(n_rows // tile,),
        out_shape=(
            jax.ShapeDtypeStruct((n_rows, PIV), f32),
            jax.ShapeDtypeStruct((n_rows, n_cols), f32),
        ),
        in_specs=[vmem] * 4,
        out_specs=(
            pl.BlockSpec((tile, PIV), lambda t: (t, 0)),
            pl.BlockSpec((tile, n_cols), lambda t: (t, 0)),
        ),
        scratch_shapes=[
            pltpu.VMEM((PIV, PIV), f32),
            pltpu.VMEM((128, PIV), bf16),
            pltpu.VMEM((3, PIV, PIV), bf16),
            pltpu.VMEM((3, PIV, n_cols), bf16),
        ],
        compiler_params=pltpu.CompilerParams(vmem_limit_bytes=32 << 20),
    )(pid, pt, fr, fc)


MESH = pl.DeviceIdType.MESH
NX = 4


def loop(lo, hi, f):
    def body(i, carry):
        f(i)
        return carry
    lax.fori_loop(lo, hi, body, 0)


def unpack(buf_ref, out_ref):
    k = buf_ref.shape[0]
    tiles = k // 4
    lane = lax.broadcasted_iota(jnp.int32, (4 * tiles, 128), 1) // 32
    quads = []
    for q in range(4):
        quads.append(jnp.concatenate([buf_ref[4 * t + q] for t in range(tiles)], axis=0))
    for g in range(4):
        acc = quads[g]
        for q in range(4):
            if q != g:
                acc = jnp.where(lane == q, pltpu.roll(quads[q], (32 * (q - g)) % 128, 1), acc)
        for t in range(tiles):
            out_ref[4 * g:4 * g + 4, 128 * t:128 * t + 128] = acc[4 * t:4 * t + 4]


def gather_kernel(nz, ny, pts_hbm, pf_hbm, ps_hbm, pid_out, piv_out, fr_out, fc_out,
                  pts_ref, in_sem, own, contrib, c_buf, x_src, x_buf, y_src, y_buf, z_src, z_buf,
                  row_buf, col_buf, rt_ref, ct_ref,
                  c_send, c_recv, x_send, x_recv, y_send, y_recv, z_send, z_recv, ag_send, ag_recv,
                  row_send, row_recv, col_send, col_recv):
    n_row, n_col = 2 * nz, ny * NX
    row = lax.axis_index("row")
    col = lax.axis_index("col")
    core, z = row % 2, row // 2
    x, y = col % NX, col // NX
    other = (2 * z + 1 - core, col)

    def x_dev(d):
        return (row, NX * y + (x + d) % NX)

    def y_dev(d):
        return (row, NX * ((y + d) % ny) + x)

    def z_dev(d):
        return (2 * ((z + d) % nz) + core, col)

    def row_dev(d):
        return (row, (col + d) % n_col)

    wide = n_col // n_row
    per = n_col // wide
    target = wide * row + col // per
    part = col % per
    source = col // wide
    first = (col % wide) * per

    arrivals = [
        pltpu.make_async_copy(pts_hbm, pts_ref, in_sem.at[0]),
        pltpu.make_async_copy(pf_hbm, pid_out.at[:, pl.ds(0, BLOCK)], in_sem.at[1]),
        pltpu.make_async_copy(ps_hbm, pid_out.at[:, pl.ds(BLOCK, BLOCK)], in_sem.at[2]),
    ]
    for a in arrivals:
        a.start()
    barrier = pltpu.get_barrier_semaphore()

    def signal(dev):
        pl.semaphore_signal(barrier, inc=1, device_id=dev, device_id_type=MESH)

    signal(other)
    loop(1, nz, lambda d: signal(z_dev(d)))
    loop(1, n_col, lambda d: signal(row_dev(d)))

    def greet_source(i):
        @pl.when(jnp.logical_or(source != row, first + i != col))
        def _():
            signal((source, first + i))

    loop(0, per, greet_source)

    for a in arrivals:
        a.wait()
    pts = pts_ref[...]
    n = pts.shape[1]
    for g in range(4):
        own[:, 32 * g:32 * g + 32] = pts[4 * g:4 * g + 4, :]
    mine = (row * n_col + col) * n
    h, m, l = split3(pts)
    for half in range(2):
        hit = pid_out[:, BLOCK * half:BLOCK * half + BLOCK] == mine + lax.broadcasted_iota(jnp.int32, (n, BLOCK), 0)
        hot = jnp.where(hit, 1.0, 0.0).astype(bf16)
        contrib[half] = (dot(l, hot) + dot(m, hot)) + dot(h, hot)
    row_buf[col] = own[...]

    to_me = n_row - 1 + jnp.where(target == col, 0, 1)
    pl.semaphore_wait(barrier, 1 + (nz - 1) + (n_col - 1) + to_me)

    def remote(src, dst, send, recv, dev):
        return pltpu.make_async_remote_copy(
            src_ref=src, dst_ref=dst, send_sem=send, recv_sem=recv, device_id=dev, device_id_type=MESH)

    def c_copy():
        return remote(contrib.at[1 - core], c_buf, c_send, c_recv, other)

    def x_copy(d):
        return remote(x_src, x_buf.at[d - 1], x_send.at[d - 1], x_recv.at[d - 1], x_dev(d))

    def y_copy(d):
        return remote(y_src, y_buf.at[d - 1], y_send.at[d - 1], y_recv.at[d - 1], y_dev(d))

    def z_copy(d):
        return remote(z_src, z_buf.at[d - 1], z_send.at[d - 1], z_recv.at[d - 1], z_dev(d))

    def ag_copy():
        return remote(piv_out.at[core], piv_out.at[core], ag_send, ag_recv, other)

    def row_copy(d):
        return remote(own, row_buf.at[col], row_send.at[d - 1], row_recv.at[d - 1], row_dev(d))

    def col_copy(d):
        return remote(own, col_buf.at[part], col_send.at[d], col_recv.at[part], ((row + d) % n_row, target))

    def col_arrival(i):
        return remote(own, col_buf.at[i], col_send.at[0], col_recv.at[i], (row, col))

    c_copy().start()
    loop(1, n_col, lambda d: row_copy(d).start())

    @pl.when(target != col)
    def _():
        col_copy(0).start()

    @pl.when(target == col)
    def _():
        col_buf[part] = own[...]

    loop(1, n_row, lambda d: col_copy(d).start())

    c_copy().wait_recv()
    total = contrib[core] + c_buf[...]
    x_src[...] = total
    for d in range(1, NX):
        x_copy(d).start()
    for d in range(1, NX):
        x_copy(d).wait_recv()
        total = total + x_buf[d - 1]
    y_src[...] = total
    for d in range(1, ny):
        y_copy(d).start()
    for d in range(1, ny):
        y_copy(d).wait_recv()
        total = total + y_buf[d - 1]
    z_src[...] = total
    for d in range(1, nz):
        z_copy(d).start()

    loop(1, n_col, lambda d: row_copy(d).wait_recv())

    def take(i):
        @pl.when(jnp.logical_or(source != row, first + i != col))
        def _():
            col_arrival(i).wait_recv()

    loop(0, per, take)
    unpack(row_buf, rt_ref)
    unpack(col_buf, ct_ref)
    fr_out[...] = features(rt_ref[...], True).T
    fc_out[...] = features(ct_ref[...], False)

    for d in range(1, nz):
        z_copy(d).wait_recv()
        total = total + z_buf[d - 1]
    piv_out[core] = total
    ag_copy().start()
    c_copy().wait_send()
    for d in range(1, NX):
        x_copy(d).wait_send()
    for d in range(1, ny):
        y_copy(d).wait_send()
    for d in range(1, nz):
        z_copy(d).wait_send()
    loop(1, n_col, lambda d: row_copy(d).wait_send())

    @pl.when(target != col)
    def _():
        col_copy(0).wait_send()

    loop(1, n_row, lambda d: col_copy(d).wait_send())
    ag_copy().wait_recv()
    ag_copy().wait_send()


def gather(points, pf, ps, mesh):
    n_row, n_col = mesh.shape["row"], mesh.shape["col"]
    nz = n_row // 2
    ny = n_col // NX
    n = points.shape[1]
    dma = pltpu.SemaphoreType.DMA
    vmem = pl.BlockSpec(memory_space=pltpu.VMEM)
    return pl.pallas_call(
        functools.partial(gather_kernel, nz, ny),
        out_shape=(
            pltpu.VMEM((1, PIV), jnp.int32),
            pltpu.VMEM((2, DIM, BLOCK), f32),
            pltpu.VMEM((n * n_col, 128), bf16),
            pltpu.VMEM((128, n * n_row), bf16),
        ),
        in_specs=[pl.BlockSpec(memory_space=pltpu.HBM)] * 3,
        out_specs=(vmem,) * 4,
        scratch_shapes=[
            pltpu.VMEM((DIM, n), f32),
            dma((3,)),
            pltpu.VMEM((4, 128), f32),
            pltpu.VMEM((2, DIM, BLOCK), f32),
            pltpu.VMEM((DIM, BLOCK), f32),
            pltpu.VMEM((DIM, BLOCK), f32),
            pltpu.VMEM((NX - 1, DIM, BLOCK), f32),
            pltpu.VMEM((DIM, BLOCK), f32),
            pltpu.VMEM((ny - 1, DIM, BLOCK), f32),
            pltpu.VMEM((DIM, BLOCK), f32),
            pltpu.VMEM((nz - 1, DIM, BLOCK), f32),
            pltpu.VMEM((n_col, 4, 128), f32),
            pltpu.VMEM((n_row, 4, 128), f32),
            pltpu.VMEM((DIM, n * n_col), f32),
            pltpu.VMEM((DIM, n * n_row), f32),
            dma, dma,
            dma((NX - 1,)), dma((NX - 1,)),
            dma((ny - 1,)), dma((ny - 1,)),
            dma((nz - 1,)), dma((nz - 1,)),
            dma, dma,
            dma((n_col - 1,)), dma((n_col - 1,)),
            dma((n_row,)), dma((n_row,)),
        ],
        compiler_params=pltpu.CompilerParams(
            collective_id=0, has_side_effects=True, vmem_limit_bytes=8 << 20),
    )(points, pf, ps)


def solution(mesh):
    def per_device(points, pivots_first, pivots_second):
        points, pf, ps = (
            pltpu.with_memory_space_constraint(x, pltpu.HBM)
            for x in (points, pivots_first[None, :], pivots_second[None, :]))
        return compute(*gather(points, pf, ps, mesh))

    return jax.shard_map(
        per_device,
        mesh=mesh,
        in_specs=(P(None, ("row", "col")), P(), P()),
        out_specs=(P("row", None), P("row", "col")),
        check_vma=False,
    )
```

```python
import functools
import jax
import jax.numpy as jnp
from jax import lax
from jax.sharding import PartitionSpec as P
from jax.experimental import pallas as pl
from jax.experimental.pallas import tpu as pltpu

DIM = 16
BLOCK = 128
PIV = 2 * BLOCK
LEAF = 32
SUB = 16
bf16 = jnp.bfloat16
f32 = jnp.float32


def split3(x):
    hi = x.astype(bf16)
    r = x - hi.astype(f32)
    mid = r.astype(bf16)
    lo = (r - mid.astype(f32)).astype(bf16)
    return hi, mid, lo


def dot(a, b):
    return lax.dot_general(a, b, (((1,), (0,)), ((), ())), preferred_element_type=f32)


def features(pts, left):
    n = pts.shape[1]
    sq = jnp.sum(pts * pts, axis=0, keepdims=True) * (-1.0 / DIM)
    sh, sm, sl = split3(sq)
    if not left:
        pts = pts * (2.0 / DIM)
    h, m, l = split3(pts)
    row = lax.broadcasted_iota(jnp.int32, (DIM, n), 0)
    at = 0 if left else 3
    ext = jnp.where((row >= 3 - at) & (row < 6 - at), 1.0, 0.0).astype(f32)
    for i, part in enumerate((sh, sm, sl)):
        ext = jnp.where(row == at + i, jnp.broadcast_to(part.astype(f32), (DIM, n)), ext)
    ext = ext.astype(bf16)
    zero = jnp.zeros((DIM, n), bf16)
    parts = (h, h, m, m, h, l, ext, zero) if left else (h, m, h, m, l, h, ext, zero)
    return jnp.concatenate(parts, axis=0)


def leaf(a_ref, o):
    G, H = LEAF // 8, PIV // 128
    rows = a_ref[pl.ds(o, LEAF), :]
    r = [[rows[8 * g:8 * g + 8, 128 * h:128 * h + 128] for h in range(H)] for g in range(G)]
    sub = lax.broadcasted_iota(jnp.int32, (8, 128), 0)
    lane = lax.broadcasted_iota(jnp.int32, (8, 128), 1)
    diag = [None] * LEAF

    def row_of(x, i):
        return jnp.broadcast_to(x[i:i + 1, :], (8, 128))

    for s in range(0, LEAF, SUB):
        h0, w = (o + s) // 128, (o + s) % 128
        v = [[None if g < s // 8 else jnp.broadcast_to(r[g][h0][:, w + m:w + m + 1], (8, 128))
              for g in range(G)] for m in range(SUB)]
        inside = (lane >= w) & (lane < w + SUB)
        for g in range(s // 8, G):
            unit = jnp.where(lane == sub + w + 8 * g - s, 1.0, 0.0)
            r[g][h0] = jnp.where(inside, unit, r[g][h0])
        for c in range(0, SUB, 2):
            g0, i0 = (s + c) // 8, (s + c) % 8
            a, b, e = row_of(v[c][g0], i0), row_of(v[c + 1][g0], i0), row_of(v[c + 1][g0], i0 + 1)
            det = a * e - b * b
            inv = 1.0 / det
            m1, m2 = {}, {}
            for g in range(g0, G):
                p, q = v[c][g], v[c + 1][g]
                if g == g0:
                    if i0 == 6:
                        continue
                    p, q = jnp.where(sub > i0 + 1, p, 0.0), jnp.where(sub > i0 + 1, q, 0.0)
                m1[g] = (p * e - q * b) * inv
                m2[g] = (q * a - p * b) * inv
            for m in range(c + 2, SUB):
                p, q = row_of(v[m][g0], i0), row_of(v[m][g0], i0 + 1)
                for g in m1:
                    v[m][g] = (v[m][g] - m1[g] * p) - m2[g] * q
            ia = 1.0 / a
            second = jnp.where(sub == i0 + 1, b * ia, 0.0)
            for h in range(H):
                p, q = row_of(r[g0][h], i0), row_of(r[g0][h], i0 + 1)
                for g in m1:
                    r[g][h] = (r[g][h] - m1[g] * p) - m2[g] * q
                r[g0][h] = r[g0][h] - second * p
            diag[s + c], diag[s + c + 1] = a, det * ia
    out = []
    for g in range(G):
        d = diag[8 * g]
        for i in range(1, 8):
            d = jnp.where(sub == i, diag[8 * g + i], d)
        scale = lax.rsqrt(d)
        h0, w = o // 128, o % 128
        done = 8 * g // SUB * SUB + SUB
        if done < LEAF:
            r[g][h0] = jnp.where((lane >= w + done) & (lane < w + LEAF), 0.0, r[g][h0])
        out.append(jnp.concatenate([x * scale for x in r[g]], axis=1))
    return jnp.concatenate(out, axis=0)


def factor(a_ref):
    for k in range(PIV // LEAF):
        o = k * LEAF
        u = leaf(a_ref, o)
        lane = lax.broadcasted_iota(jnp.int32, (LEAF, PIV), 1)
        a_ref[pl.ds(o, LEAF), :] = jnp.where(lane < o + LEAF, u, 0.0)
        left = PIV - o - LEAF
        if left:
            h, m, l = split3(u)
            lhs = jnp.concatenate((h, h, m, m, h, l), axis=0)
            rhs = jnp.concatenate((h, m, h, m, l, h), axis=0)
            start = ((o + LEAF) // 128) * 128
            lt = lhs[:, start:].T
            lt = lt[o + LEAF - start:, :]
            upd = dot(lt, rhs)
            lane = lax.broadcasted_iota(jnp.int32, (left, PIV), 1)
            old = a_ref[pl.ds(o + LEAF, left), :]
            old = jnp.where((lane >= o) & (lane < o + LEAF), 0.0, old)
            a_ref[pl.ds(o + LEAF, left), :] = old - upd


def dot_t(a, b):
    return lax.dot_general(a, b, (((1,), (1,)), ((), ())), preferred_element_type=f32)


def dot6(ls, rs, dot=dot):
    lh, lm, ll = ls
    rh, rm, rl = rs
    return (dot(ll, rh) + dot(lh, rl) + dot(lm, rm)) + (dot(lm, rh) + dot(lh, rm)) + dot(lh, rh)


def dot3(ls, rs):
    lh, lm = ls[:2]
    rh, rm = rs[:2]
    return (dot(lm, rh) + dot(lh, rm)) + dot(lh, rh)


def kernel_b(pid_ref, pt_ref, fr_ref, fc_ref, panel_ref, schur_ref,
             a_ref, fp_ref, wt_ref, pc_ref, *, tile):
    t = pl.program_id(0)
    n_cols = fc_ref.shape[1]
    row0 = lax.axis_index("row") * fr_ref.shape[0] + t * tile
    col0 = lax.axis_index("col") * n_cols
    piv = pid_ref[...]

    @pl.when(t == 0)
    def _():
        pt = jnp.concatenate([pt_ref[0], pt_ref[1]], axis=1)
        fp = features(pt, False)
        fp_ref[...] = fp
        fpl = features(pt, True).T
        kpp = jnp.exp(dot(fpl, fp))
        i = lax.broadcasted_iota(jnp.int32, (PIV, PIV), 0)
        j = lax.broadcasted_iota(jnp.int32, (PIV, PIV), 1)
        a_ref[...] = jnp.where(i == j, kpp + 0.1, kpp)
        kpc = jnp.exp(dot(fpl, fc_ref[...]))
        ids = jnp.broadcast_to(piv.astype(f32), (8, PIV)).T[:, 0:1].astype(jnp.int32)
        cid = col0 + lax.broadcasted_iota(jnp.int32, (PIV, n_cols), 1)
        kpc = kpc + jnp.where(cid == ids, 0.1, 0.0)
        factor(a_ref)
        w = a_ref[...]
        ws = split3(w)
        for q, x in enumerate(ws):
            wt_ref[q] = x
        pc = dot6(ws, split3(kpc))
        for q, x in enumerate(split3(pc)):
            pc_ref[q] = x

    fr = fr_ref[pl.ds(pl.multiple_of(t * tile, tile), tile), :]
    krp = jnp.exp(dot(fr, fp_ref[...]))
    rid = row0 + lax.broadcasted_iota(jnp.int32, (tile, PIV), 0)
    krp = krp + jnp.where(rid == piv, 0.1, 0.0)
    panel = dot6(split3(krp), (wt_ref[0], wt_ref[1], wt_ref[2]), dot_t)
    panel_ref[...] = panel
    krc = jnp.exp(dot(fr, fc_ref[...]))
    i = lax.broadcasted_iota(jnp.int32, (tile, n_cols), 0)
    j = lax.broadcasted_iota(jnp.int32, (tile, n_cols), 1)
    krc = krc + jnp.where(i - j == col0 - row0, 0.1, 0.0)
    schur_ref[...] = krc - dot6(split3(panel), (pc_ref[0], pc_ref[1], pc_ref[2]))


def compute(pid, pt, fr, fc, tile=512):
    n_rows, n_cols = fr.shape[0], fc.shape[1]
    vmem = pl.BlockSpec(memory_space=pltpu.VMEM)
    return pl.pallas_call(
        functools.partial(kernel_b, tile=tile),
        grid=(n_rows // tile,),
        out_shape=(
            jax.ShapeDtypeStruct((n_rows, PIV), f32),
            jax.ShapeDtypeStruct((n_rows, n_cols), f32),
        ),
        in_specs=[vmem] * 4,
        out_specs=(
            pl.BlockSpec((tile, PIV), lambda t: (t, 0)),
            pl.BlockSpec((tile, n_cols), lambda t: (t, 0)),
        ),
        scratch_shapes=[
            pltpu.VMEM((PIV, PIV), f32),
            pltpu.VMEM((128, PIV), bf16),
            pltpu.VMEM((3, PIV, PIV), bf16),
            pltpu.VMEM((3, PIV, n_cols), bf16),
        ],
        compiler_params=pltpu.CompilerParams(vmem_limit_bytes=32 << 20),
    )(pid, pt, fr, fc)


MESH = pl.DeviceIdType.MESH
NX = 4


def loop(lo, hi, f):
    def body(i, carry):
        f(i)
        return carry
    lax.fori_loop(lo, hi, body, 0)


def unpack(buf_ref, out_ref):
    k = buf_ref.shape[0]
    tiles = k // 4
    lane = lax.broadcasted_iota(jnp.int32, (4 * tiles, 128), 1) // 32
    quads = []
    for q in range(4):
        quads.append(jnp.concatenate([buf_ref[4 * t + q] for t in range(tiles)], axis=0))
    for g in range(4):
        acc = quads[g]
        for q in range(4):
            if q != g:
                acc = jnp.where(lane == q, pltpu.roll(quads[q], (32 * (q - g)) % 128, 1), acc)
        for t in range(tiles):
            out_ref[4 * g:4 * g + 4, 128 * t:128 * t + 128] = acc[4 * t:4 * t + 4]


def gather_kernel(nz, ny, pts_hbm, pf_hbm, ps_hbm, pid_out, piv_out, fr_out, fc_out,
                  pts_ref, in_sem, own, contrib, c_buf, x_src, x_buf, y_src, y_buf, z_src, z_buf,
                  row_buf, col_buf, rt_ref, ct_ref,
                  c_send, c_recv, x_send, x_recv, y_send, y_recv, z_send, z_recv, ag_send, ag_recv,
                  row_send, row_recv, col_send, col_recv):
    n_row, n_col = 2 * nz, ny * NX
    row = lax.axis_index("row")
    col = lax.axis_index("col")
    core, z = row % 2, row // 2
    x, y = col % NX, col // NX
    other = (2 * z + 1 - core, col)

    def x_dev(d):
        return (row, NX * y + (x + d) % NX)

    def y_dev(d):
        return (row, NX * ((y + d) % ny) + x)

    def z_dev(d):
        return (2 * ((z + d) % nz) + core, col)

    def row_dev(d):
        return (row, (col + d) % n_col)

    wide = n_col // n_row
    per = n_col // wide
    target = wide * row + col // per
    part = col % per
    source = col // wide
    first = (col % wide) * per

    arrivals = [
        pltpu.make_async_copy(pts_hbm, pts_ref, in_sem.at[0]),
        pltpu.make_async_copy(pf_hbm, pid_out.at[:, pl.ds(0, BLOCK)], in_sem.at[1]),
        pltpu.make_async_copy(ps_hbm, pid_out.at[:, pl.ds(BLOCK, BLOCK)], in_sem.at[2]),
    ]
    for a in arrivals:
        a.start()
    barrier = pltpu.get_barrier_semaphore()

    def signal(dev):
        pl.semaphore_signal(barrier, inc=1, device_id=dev, device_id_type=MESH)

    signal(other)
    loop(1, nz, lambda d: signal(z_dev(d)))
    loop(1, n_col, lambda d: signal(row_dev(d)))

    def greet_source(i):
        @pl.when(jnp.logical_or(source != row, first + i != col))
        def _():
            signal((source, first + i))

    loop(0, per, greet_source)

    for a in arrivals:
        a.wait()
    pts = pts_ref[...]
    n = pts.shape[1]
    for g in range(4):
        own[:, 32 * g:32 * g + 32] = pts[4 * g:4 * g + 4, :]
    mine = (row * n_col + col) * n
    h, m, l = split3(pts)
    for half in range(2):
        hit = pid_out[:, BLOCK * half:BLOCK * half + BLOCK] == mine + lax.broadcasted_iota(jnp.int32, (n, BLOCK), 0)
        hot = jnp.where(hit, 1.0, 0.0).astype(bf16)
        contrib[half] = (dot(l, hot) + dot(m, hot)) + dot(h, hot)
    row_buf[col] = own[...]

    to_me = n_row - 1 + jnp.where(target == col, 0, 1)
    pl.semaphore_wait(barrier, 1 + (nz - 1) + (n_col - 1) + to_me)

    def remote(src, dst, send, recv, dev):
        return pltpu.make_async_remote_copy(
            src_ref=src, dst_ref=dst, send_sem=send, recv_sem=recv, device_id=dev, device_id_type=MESH)

    def c_copy():
        return remote(contrib.at[1 - core], c_buf, c_send, c_recv, other)

    def x_copy(d):
        return remote(x_src, x_buf.at[d - 1], x_send.at[d - 1], x_recv.at[d - 1], x_dev(d))

    def y_copy(d):
        return remote(y_src, y_buf.at[d - 1], y_send.at[d - 1], y_recv.at[d - 1], y_dev(d))

    def z_copy(d):
        return remote(z_src, z_buf.at[d - 1], z_send.at[d - 1], z_recv.at[d - 1], z_dev(d))

    def ag_copy():
        return remote(piv_out.at[core], piv_out.at[core], ag_send, ag_recv, other)

    def row_copy(d):
        return remote(own, row_buf.at[col], row_send.at[d - 1], row_recv.at[d - 1], row_dev(d))

    def col_copy(d):
        return remote(own, col_buf.at[part], col_send.at[d], col_recv.at[part], ((row + d) % n_row, target))

    def col_arrival(i):
        return remote(own, col_buf.at[i], col_send.at[0], col_recv.at[i], (row, col))

    c_copy().start()
    loop(1, n_col, lambda d: row_copy(d).start())

    @pl.when(target != col)
    def _():
        col_copy(0).start()

    @pl.when(target == col)
    def _():
        col_buf[part] = own[...]

    loop(1, n_row, lambda d: col_copy(d).start())

    c_copy().wait_recv()
    total = contrib[core] + c_buf[...]
    x_src[...] = total
    for d in range(1, NX):
        x_copy(d).start()
    for d in range(1, NX):
        x_copy(d).wait_recv()
        total = total + x_buf[d - 1]
    y_src[...] = total
    for d in range(1, ny):
        y_copy(d).start()
    for d in range(1, ny):
        y_copy(d).wait_recv()
        total = total + y_buf[d - 1]
    z_src[...] = total
    for d in range(1, nz):
        z_copy(d).start()

    loop(1, n_col, lambda d: row_copy(d).wait_recv())

    def take(i):
        @pl.when(jnp.logical_or(source != row, first + i != col))
        def _():
            col_arrival(i).wait_recv()

    loop(0, per, take)
    unpack(row_buf, rt_ref)
    unpack(col_buf, ct_ref)
    fr_out[...] = features(rt_ref[...], True).T
    fc_out[...] = features(ct_ref[...], False)

    for d in range(1, nz):
        z_copy(d).wait_recv()
        total = total + z_buf[d - 1]
    piv_out[core] = total
    ag_copy().start()
    c_copy().wait_send()
    for d in range(1, NX):
        x_copy(d).wait_send()
    for d in range(1, ny):
        y_copy(d).wait_send()
    for d in range(1, nz):
        z_copy(d).wait_send()
    loop(1, n_col, lambda d: row_copy(d).wait_send())

    @pl.when(target != col)
    def _():
        col_copy(0).wait_send()

    loop(1, n_row, lambda d: col_copy(d).wait_send())
    ag_copy().wait_recv()
    ag_copy().wait_send()


def gather(points, pf, ps, mesh):
    n_row, n_col = mesh.shape["row"], mesh.shape["col"]
    nz = n_row // 2
    ny = n_col // NX
    n = points.shape[1]
    dma = pltpu.SemaphoreType.DMA
    vmem = pl.BlockSpec(memory_space=pltpu.VMEM)
    return pl.pallas_call(
        functools.partial(gather_kernel, nz, ny),
        out_shape=(
            pltpu.VMEM((1, PIV), jnp.int32),
            pltpu.VMEM((2, DIM, BLOCK), f32),
            pltpu.VMEM((n * n_col, 128), bf16),
            pltpu.VMEM((128, n * n_row), bf16),
        ),
        in_specs=[pl.BlockSpec(memory_space=pltpu.HBM)] * 3,
        out_specs=(vmem,) * 4,
        scratch_shapes=[
            pltpu.VMEM((DIM, n), f32),
            dma((3,)),
            pltpu.VMEM((4, 128), f32),
            pltpu.VMEM((2, DIM, BLOCK), f32),
            pltpu.VMEM((DIM, BLOCK), f32),
            pltpu.VMEM((DIM, BLOCK), f32),
            pltpu.VMEM((NX - 1, DIM, BLOCK), f32),
            pltpu.VMEM((DIM, BLOCK), f32),
            pltpu.VMEM((ny - 1, DIM, BLOCK), f32),
            pltpu.VMEM((DIM, BLOCK), f32),
            pltpu.VMEM((nz - 1, DIM, BLOCK), f32),
            pltpu.VMEM((n_col, 4, 128), f32),
            pltpu.VMEM((n_row, 4, 128), f32),
            pltpu.VMEM((DIM, n * n_col), f32),
            pltpu.VMEM((DIM, n * n_row), f32),
            dma, dma,
            dma((NX - 1,)), dma((NX - 1,)),
            dma((ny - 1,)), dma((ny - 1,)),
            dma((nz - 1,)), dma((nz - 1,)),
            dma, dma,
            dma((n_col - 1,)), dma((n_col - 1,)),
            dma((n_row,)), dma((n_row,)),
        ],
        compiler_params=pltpu.CompilerParams(
            collective_id=0, has_side_effects=True, vmem_limit_bytes=8 << 20),
    )(points, pf, ps)


def solution(mesh):
    def per_device(points, pivots_first, pivots_second):
        points, pf, ps = (
            pltpu.with_memory_space_constraint(x, pltpu.HBM)
            for x in (points, pivots_first[None, :], pivots_second[None, :]))
        return compute(*gather(points, pf, ps, mesh))

    return jax.shard_map(
        per_device,
        mesh=mesh,
        in_specs=(P(None, ("row", "col")), P(), P()),
        out_specs=(P("row", None), P("row", "col")),
        check_vma=False,
    )
```

```python
import functools
import jax
import jax.numpy as jnp
from jax import lax
from jax.sharding import PartitionSpec as P
from jax.experimental import pallas as pl
from jax.experimental.pallas import tpu as pltpu

DIM = 16
BLOCK = 128
PIV = 2 * BLOCK
LEAF = 32
SUB = 16
bf16 = jnp.bfloat16
f32 = jnp.float32


def split3(x):
    hi = x.astype(bf16)
    r = x - hi.astype(f32)
    mid = r.astype(bf16)
    lo = (r - mid.astype(f32)).astype(bf16)
    return hi, mid, lo


def dot(a, b):
    return lax.dot_general(a, b, (((1,), (0,)), ((), ())), preferred_element_type=f32)


def features(pts, left):
    n = pts.shape[1]
    sq = jnp.sum(pts * pts, axis=0, keepdims=True) * (-1.0 / DIM)
    sh, sm, sl = split3(sq)
    if not left:
        pts = pts * (2.0 / DIM)
    h, m, l = split3(pts)
    row = lax.broadcasted_iota(jnp.int32, (DIM, n), 0)
    at = 0 if left else 3
    ext = jnp.where((row >= 3 - at) & (row < 6 - at), 1.0, 0.0).astype(f32)
    for i, part in enumerate((sh, sm, sl)):
        ext = jnp.where(row == at + i, jnp.broadcast_to(part.astype(f32), (DIM, n)), ext)
    ext = ext.astype(bf16)
    zero = jnp.zeros((DIM, n), bf16)
    parts = (h, h, m, m, h, l, ext, zero) if left else (h, m, h, m, l, h, ext, zero)
    return jnp.concatenate(parts, axis=0)


def leaf(a_ref, o):
    G, H = LEAF // 8, PIV // 128
    rows = a_ref[pl.ds(o, LEAF), :]
    r = [[rows[8 * g:8 * g + 8, 128 * h:128 * h + 128] for h in range(H)] for g in range(G)]
    sub = lax.broadcasted_iota(jnp.int32, (8, 128), 0)
    lane = lax.broadcasted_iota(jnp.int32, (8, 128), 1)
    diag = [None] * LEAF

    def row_of(x, i):
        return jnp.broadcast_to(x[i:i + 1, :], (8, 128))

    for s in range(0, LEAF, SUB):
        h0, w = (o + s) // 128, (o + s) % 128
        v = [[None if g < s // 8 else jnp.broadcast_to(r[g][h0][:, w + m:w + m + 1], (8, 128))
              for g in range(G)] for m in range(SUB)]
        inside = (lane >= w) & (lane < w + SUB)
        for g in range(s // 8, G):
            unit = jnp.where(lane == sub + w + 8 * g - s, 1.0, 0.0)
            r[g][h0] = jnp.where(inside, unit, r[g][h0])
        for c in range(0, SUB, 2):
            g0, i0 = (s + c) // 8, (s + c) % 8
            a, b, e = row_of(v[c][g0], i0), row_of(v[c + 1][g0], i0), row_of(v[c + 1][g0], i0 + 1)
            det = a * e - b * b
            inv = 1.0 / det
            m1, m2 = {}, {}
            for g in range(g0, G):
                p, q = v[c][g], v[c + 1][g]
                if g == g0:
                    if i0 == 6:
                        continue
                    p, q = jnp.where(sub > i0 + 1, p, 0.0), jnp.where(sub > i0 + 1, q, 0.0)
                m1[g] = (p * e - q * b) * inv
                m2[g] = (q * a - p * b) * inv
            for m in range(c + 2, SUB):
                p, q = row_of(v[m][g0], i0), row_of(v[m][g0], i0 + 1)
                for g in m1:
                    v[m][g] = (v[m][g] - m1[g] * p) - m2[g] * q
            ia = 1.0 / a
            second = jnp.where(sub == i0 + 1, b * ia, 0.0)
            for h in range(H):
                p, q = row_of(r[g0][h], i0), row_of(r[g0][h], i0 + 1)
                for g in m1:
                    r[g][h] = (r[g][h] - m1[g] * p) - m2[g] * q
                r[g0][h] = r[g0][h] - second * p
            diag[s + c], diag[s + c + 1] = a, det * ia
    out = []
    for g in range(G):
        d = diag[8 * g]
        for i in range(1, 8):
            d = jnp.where(sub == i, diag[8 * g + i], d)
        scale = lax.rsqrt(d)
        h0, w = o // 128, o % 128
        done = 8 * g // SUB * SUB + SUB
        if done < LEAF:
            r[g][h0] = jnp.where((lane >= w + done) & (lane < w + LEAF), 0.0, r[g][h0])
        out.append(jnp.concatenate([x * scale for x in r[g]], axis=1))
    return jnp.concatenate(out, axis=0)


def factor(a_ref):
    for k in range(PIV // LEAF):
        o = k * LEAF
        u = leaf(a_ref, o)
        lane = lax.broadcasted_iota(jnp.int32, (LEAF, PIV), 1)
        a_ref[pl.ds(o, LEAF), :] = jnp.where(lane < o + LEAF, u, 0.0)
        left = PIV - o - LEAF
        if left:
            h, m, l = split3(u)
            lhs = jnp.concatenate((h, h, m, m, h, l), axis=0)
            rhs = jnp.concatenate((h, m, h, m, l, h), axis=0)
            start = ((o + LEAF) // 128) * 128
            lt = lhs[:, start:].T
            lt = lt[o + LEAF - start:, :]
            upd = dot(lt, rhs)
            lane = lax.broadcasted_iota(jnp.int32, (left, PIV), 1)
            old = a_ref[pl.ds(o + LEAF, left), :]
            old = jnp.where((lane >= o) & (lane < o + LEAF), 0.0, old)
            a_ref[pl.ds(o + LEAF, left), :] = old - upd


def dot_t(a, b):
    return lax.dot_general(a, b, (((1,), (1,)), ((), ())), preferred_element_type=f32)


def dot6(ls, rs, dot=dot):
    lh, lm, ll = ls
    rh, rm, rl = rs
    return (dot(ll, rh) + dot(lh, rl) + dot(lm, rm)) + (dot(lm, rh) + dot(lh, rm)) + dot(lh, rh)


def dot3(ls, rs):
    lh, lm = ls[:2]
    rh, rm = rs[:2]
    return (dot(lm, rh) + dot(lh, rm)) + dot(lh, rh)


def kernel_b(pid_ref, pt_ref, fr_ref, fc_ref, krc_ref, panel_ref, schur_ref,
             a_ref, fp_ref, wt_ref, pc_ref, *, tile):
    t = pl.program_id(0)
    n_cols = fc_ref.shape[1]
    row0 = lax.axis_index("row") * fr_ref.shape[0] + t * tile
    col0 = lax.axis_index("col") * n_cols
    piv = pid_ref[...]

    @pl.when(t == 0)
    def _():
        pt = jnp.concatenate([pt_ref[0], pt_ref[1]], axis=1)
        fp = features(pt, False)
        fp_ref[...] = fp
        fpl = features(pt, True).T
        kpp = jnp.exp(dot(fpl, fp))
        i = lax.broadcasted_iota(jnp.int32, (PIV, PIV), 0)
        j = lax.broadcasted_iota(jnp.int32, (PIV, PIV), 1)
        a_ref[...] = jnp.where(i == j, kpp + 0.1, kpp)
        kpc = jnp.exp(dot(fpl, fc_ref[...]))
        ids = jnp.broadcast_to(piv.astype(f32), (8, PIV)).T[:, 0:1].astype(jnp.int32)
        cid = col0 + lax.broadcasted_iota(jnp.int32, (PIV, n_cols), 1)
        kpc = kpc + jnp.where(cid == ids, 0.1, 0.0)
        factor(a_ref)
        w = a_ref[...]
        ws = split3(w)
        for q, x in enumerate(ws):
            wt_ref[q] = x
        pc = dot6(ws, split3(kpc))
        for q, x in enumerate(split3(pc)):
            pc_ref[q] = x

    fr = fr_ref[pl.ds(pl.multiple_of(t * tile, tile), tile), :]
    krp = jnp.exp(dot(fr, fp_ref[...]))
    rid = row0 + lax.broadcasted_iota(jnp.int32, (tile, PIV), 0)
    krp = krp + jnp.where(rid == piv, 0.1, 0.0)
    panel = dot6(split3(krp), (wt_ref[0], wt_ref[1], wt_ref[2]), dot_t)
    panel_ref[...] = panel
    krc = krc_ref[pl.ds(pl.multiple_of(t * tile, tile), tile), :]
    schur_ref[...] = krc - dot6(split3(panel), (pc_ref[0], pc_ref[1], pc_ref[2]))


def compute(pid, pt, fr, fc, krc, tile=512):
    n_rows, n_cols = fr.shape[0], fc.shape[1]
    vmem = pl.BlockSpec(memory_space=pltpu.VMEM)
    return pl.pallas_call(
        functools.partial(kernel_b, tile=tile),
        grid=(n_rows // tile,),
        out_shape=(
            jax.ShapeDtypeStruct((n_rows, PIV), f32),
            jax.ShapeDtypeStruct((n_rows, n_cols), f32),
        ),
        in_specs=[vmem] * 5,
        out_specs=(
            pl.BlockSpec((tile, PIV), lambda t: (t, 0)),
            pl.BlockSpec((tile, n_cols), lambda t: (t, 0)),
        ),
        scratch_shapes=[
            pltpu.VMEM((PIV, PIV), f32),
            pltpu.VMEM((128, PIV), bf16),
            pltpu.VMEM((3, PIV, PIV), bf16),
            pltpu.VMEM((3, PIV, n_cols), bf16),
        ],
        compiler_params=pltpu.CompilerParams(vmem_limit_bytes=32 << 20),
    )(pid, pt, fr, fc, krc)


MESH = pl.DeviceIdType.MESH
NX = 4


def loop(lo, hi, f):
    def body(i, carry):
        f(i)
        return carry
    lax.fori_loop(lo, hi, body, 0)


def unpack(buf_ref, out_ref):
    k = buf_ref.shape[0]
    tiles = k // 4
    lane = lax.broadcasted_iota(jnp.int32, (4 * tiles, 128), 1) // 32
    quads = []
    for q in range(4):
        quads.append(jnp.concatenate([buf_ref[4 * t + q] for t in range(tiles)], axis=0))
    for g in range(4):
        acc = quads[g]
        for q in range(4):
            if q != g:
                acc = jnp.where(lane == q, pltpu.roll(quads[q], (32 * (q - g)) % 128, 1), acc)
        for t in range(tiles):
            out_ref[4 * g:4 * g + 4, 128 * t:128 * t + 128] = acc[4 * t:4 * t + 4]


def gather_kernel(nz, ny, pts_hbm, pf_hbm, ps_hbm, pid_out, piv_out, fr_out, fc_out, krc_out,
                  pts_ref, in_sem, own, contrib, c_buf, x_src, x_buf, y_src, y_buf, z_src, z_buf,
                  row_buf, col_buf, rt_ref, ct_ref,
                  c_send, c_recv, x_send, x_recv, y_send, y_recv, z_send, z_recv, ag_send, ag_recv,
                  row_send, row_recv, col_send, col_recv):
    n_row, n_col = 2 * nz, ny * NX
    row = lax.axis_index("row")
    col = lax.axis_index("col")
    core, z = row % 2, row // 2
    x, y = col % NX, col // NX
    other = (2 * z + 1 - core, col)

    def x_dev(d):
        return (row, NX * y + (x + d) % NX)

    def y_dev(d):
        return (row, NX * ((y + d) % ny) + x)

    def z_dev(d):
        return (2 * ((z + d) % nz) + core, col)

    def row_dev(d):
        return (row, (col + d) % n_col)

    wide = n_col // n_row
    per = n_col // wide
    target = wide * row + col // per
    part = col % per
    source = col // wide
    first = (col % wide) * per

    arrivals = [
        pltpu.make_async_copy(pts_hbm, pts_ref, in_sem.at[0]),
        pltpu.make_async_copy(pf_hbm, pid_out.at[:, pl.ds(0, BLOCK)], in_sem.at[1]),
        pltpu.make_async_copy(ps_hbm, pid_out.at[:, pl.ds(BLOCK, BLOCK)], in_sem.at[2]),
    ]
    for a in arrivals:
        a.start()
    barrier = pltpu.get_barrier_semaphore()

    def signal(dev):
        pl.semaphore_signal(barrier, inc=1, device_id=dev, device_id_type=MESH)


    def greet_source(i):
        @pl.when(jnp.logical_or(source != row, first + i != col))
        def _():
            signal((source, first + i))

    loop(0, per, greet_source)
    loop(1, nz, lambda d: signal(z_dev(d)))
    loop(1, n_col, lambda d: signal(row_dev(d)))
    signal(other)

    for a in arrivals:
        a.wait()
    pts = pts_ref[...]
    n = pts.shape[1]
    for g in range(4):
        own[:, 32 * g:32 * g + 32] = pts[4 * g:4 * g + 4, :]
    mine = (row * n_col + col) * n
    h, m, l = split3(pts)
    for half in range(2):
        hit = pid_out[:, BLOCK * half:BLOCK * half + BLOCK] == mine + lax.broadcasted_iota(jnp.int32, (n, BLOCK), 0)
        hot = jnp.where(hit, 1.0, 0.0).astype(bf16)
        contrib[half] = (dot(l, hot) + dot(m, hot)) + dot(h, hot)
    row_buf[col] = own[...]

    to_me = n_row - 1 + jnp.where(target == col, 0, 1)
    pl.semaphore_wait(barrier, 1 + (nz - 1) + (n_col - 1) + to_me)

    def remote(src, dst, send, recv, dev):
        return pltpu.make_async_remote_copy(
            src_ref=src, dst_ref=dst, send_sem=send, recv_sem=recv, device_id=dev, device_id_type=MESH)

    def c_copy():
        return remote(contrib.at[1 - core], c_buf, c_send, c_recv, other)

    def x_copy(d):
        return remote(x_src, x_buf.at[d - 1], x_send.at[d - 1], x_recv.at[d - 1], x_dev(d))

    def y_copy(d):
        return remote(y_src, y_buf.at[d - 1], y_send.at[d - 1], y_recv.at[d - 1], y_dev(d))

    def z_copy(d):
        return remote(z_src, z_buf.at[d - 1], z_send.at[d - 1], z_recv.at[d - 1], z_dev(d))

    def ag_copy():
        return remote(piv_out.at[core], piv_out.at[core], ag_send, ag_recv, other)

    def row_copy(d):
        return remote(own, row_buf.at[col], row_send.at[d - 1], row_recv.at[d - 1], row_dev(d))

    def col_copy(d):
        return remote(own, col_buf.at[part], col_send.at[d], col_recv.at[part], ((row + d) % n_row, target))

    def col_arrival(i):
        return remote(own, col_buf.at[i], col_send.at[0], col_recv.at[i], (row, col))

    c_copy().start()
    loop(1, n_col, lambda d: row_copy(d).start())

    @pl.when(target != col)
    def _():
        col_copy(0).start()

    @pl.when(target == col)
    def _():
        col_buf[part] = own[...]

    loop(1, n_row, lambda d: col_copy(d).start())

    c_copy().wait_recv()
    total = contrib[core] + c_buf[...]
    x_src[...] = total
    for d in range(1, NX):
        x_copy(d).start()
    for d in range(1, NX):
        x_copy(d).wait_recv()
        total = total + x_buf[d - 1]
    y_src[...] = total
    for d in range(1, ny):
        y_copy(d).start()
    for d in range(1, ny):
        y_copy(d).wait_recv()
        total = total + y_buf[d - 1]
    z_src[...] = total
    for d in range(1, nz):
        z_copy(d).start()

    loop(1, n_col, lambda d: row_copy(d).wait_recv())

    def take(i):
        @pl.when(jnp.logical_or(source != row, first + i != col))
        def _():
            col_arrival(i).wait_recv()

    loop(0, per, take)
    unpack(row_buf, rt_ref)
    unpack(col_buf, ct_ref)
    fr_out[...] = features(rt_ref[...], True).T
    fc_out[...] = features(ct_ref[...], False)
    n_cols = fc_out.shape[1]
    off = col * n_cols - row * fr_out.shape[0]
    step = 256

    def block(b):
        at = pl.ds(pl.multiple_of(b * step, step), step)
        i = b * step + lax.broadcasted_iota(jnp.int32, (step, n_cols), 0)
        j = off + lax.broadcasted_iota(jnp.int32, (step, n_cols), 1)
        k = jnp.exp(dot(fr_out[at, :], fc_out[...]))
        krc_out[at, :] = k + jnp.where(i == j, 0.1, 0.0)

    loop(0, fr_out.shape[0] // step, block)

    for d in range(1, nz):
        z_copy(d).wait_recv()
        total = total + z_buf[d - 1]
    piv_out[core] = total
    ag_copy().start()
    c_copy().wait_send()
    for d in range(1, NX):
        x_copy(d).wait_send()
    for d in range(1, ny):
        y_copy(d).wait_send()
    for d in range(1, nz):
        z_copy(d).wait_send()
    loop(1, n_col, lambda d: row_copy(d).wait_send())

    @pl.when(target != col)
    def _():
        col_copy(0).wait_send()

    loop(1, n_row, lambda d: col_copy(d).wait_send())
    ag_copy().wait_recv()
    ag_copy().wait_send()


def gather(points, pf, ps, mesh):
    n_row, n_col = mesh.shape["row"], mesh.shape["col"]
    nz = n_row // 2
    ny = n_col // NX
    n = points.shape[1]
    dma = pltpu.SemaphoreType.DMA
    vmem = pl.BlockSpec(memory_space=pltpu.VMEM)
    return pl.pallas_call(
        functools.partial(gather_kernel, nz, ny),
        out_shape=(
            pltpu.VMEM((1, PIV), jnp.int32),
            pltpu.VMEM((2, DIM, BLOCK), f32),
            pltpu.VMEM((n * n_col, 128), bf16),
            pltpu.VMEM((128, n * n_row), bf16),
            pltpu.VMEM((n * n_col, n * n_row), f32),
        ),
        in_specs=[pl.BlockSpec(memory_space=pltpu.HBM)] * 3,
        out_specs=(vmem,) * 5,
        scratch_shapes=[
            pltpu.VMEM((DIM, n), f32),
            dma((3,)),
            pltpu.VMEM((4, 128), f32),
            pltpu.VMEM((2, DIM, BLOCK), f32),
            pltpu.VMEM((DIM, BLOCK), f32),
            pltpu.VMEM((DIM, BLOCK), f32),
            pltpu.VMEM((NX - 1, DIM, BLOCK), f32),
            pltpu.VMEM((DIM, BLOCK), f32),
            pltpu.VMEM((ny - 1, DIM, BLOCK), f32),
            pltpu.VMEM((DIM, BLOCK), f32),
            pltpu.VMEM((nz - 1, DIM, BLOCK), f32),
            pltpu.VMEM((n_col, 4, 128), f32),
            pltpu.VMEM((n_row, 4, 128), f32),
            pltpu.VMEM((DIM, n * n_col), f32),
            pltpu.VMEM((DIM, n * n_row), f32),
            dma, dma,
            dma((NX - 1,)), dma((NX - 1,)),
            dma((ny - 1,)), dma((ny - 1,)),
            dma((nz - 1,)), dma((nz - 1,)),
            dma, dma,
            dma((n_col - 1,)), dma((n_col - 1,)),
            dma((n_row,)), dma((n_row,)),
        ],
        compiler_params=pltpu.CompilerParams(
            collective_id=0, has_side_effects=True, vmem_limit_bytes=8 << 20),
    )(points, pf, ps)


def solution(mesh):
    def per_device(points, pivots_first, pivots_second):
        points, pf, ps = (
            pltpu.with_memory_space_constraint(x, pltpu.HBM)
            for x in (points, pivots_first[None, :], pivots_second[None, :]))
        return compute(*gather(points, pf, ps, mesh))

    return jax.shard_map(
        per_device,
        mesh=mesh,
        in_specs=(P(None, ("row", "col")), P(), P()),
        out_specs=(P("row", None), P("row", "col")),
        check_vma=False,
    )
```

```python
import functools
import jax
import jax.numpy as jnp
from jax import lax
from jax.sharding import PartitionSpec as P
from jax.experimental import pallas as pl
from jax.experimental.pallas import tpu as pltpu

DIM = 16
BLOCK = 128
PIV = 2 * BLOCK
LEAF = 32
SUB = 16
bf16 = jnp.bfloat16
f32 = jnp.float32


def split3(x):
    hi = x.astype(bf16)
    r = x - hi.astype(f32)
    mid = r.astype(bf16)
    lo = (r - mid.astype(f32)).astype(bf16)
    return hi, mid, lo


def dot(a, b):
    return lax.dot_general(a, b, (((1,), (0,)), ((), ())), preferred_element_type=f32)


def features(pts, left):
    n = pts.shape[1]
    sq = jnp.sum(pts * pts, axis=0, keepdims=True) * (-1.0 / DIM)
    sh, sm, sl = split3(sq)
    if not left:
        pts = pts * (2.0 / DIM)
    h, m, l = split3(pts)
    row = lax.broadcasted_iota(jnp.int32, (DIM, n), 0)
    at = 0 if left else 3
    ext = jnp.where((row >= 3 - at) & (row < 6 - at), 1.0, 0.0).astype(f32)
    for i, part in enumerate((sh, sm, sl)):
        ext = jnp.where(row == at + i, jnp.broadcast_to(part.astype(f32), (DIM, n)), ext)
    ext = ext.astype(bf16)
    zero = jnp.zeros((DIM, n), bf16)
    parts = (h, h, m, m, h, l, ext, zero) if left else (h, m, h, m, l, h, ext, zero)
    return jnp.concatenate(parts, axis=0)


def leaf(a_ref, o):
    G, H = LEAF // 8, PIV // 128
    rows = a_ref[pl.ds(o, LEAF), :]
    r = [[rows[8 * g:8 * g + 8, 128 * h:128 * h + 128] for h in range(H)] for g in range(G)]
    sub = lax.broadcasted_iota(jnp.int32, (8, 128), 0)
    lane = lax.broadcasted_iota(jnp.int32, (8, 128), 1)
    diag = [None] * LEAF

    def row_of(x, i):
        return jnp.broadcast_to(x[i:i + 1, :], (8, 128))

    for s in range(0, LEAF, SUB):
        h0, w = (o + s) // 128, (o + s) % 128
        v = [[None if g < s // 8 else jnp.broadcast_to(r[g][h0][:, w + m:w + m + 1], (8, 128))
              for g in range(G)] for m in range(SUB)]
        inside = (lane >= w) & (lane < w + SUB)
        for g in range(s // 8, G):
            unit = jnp.where(lane == sub + w + 8 * g - s, 1.0, 0.0)
            r[g][h0] = jnp.where(inside, unit, r[g][h0])
        for c in range(0, SUB, 2):
            g0, i0 = (s + c) // 8, (s + c) % 8
            a, b, e = row_of(v[c][g0], i0), row_of(v[c + 1][g0], i0), row_of(v[c + 1][g0], i0 + 1)
            det = a * e - b * b
            inv = 1.0 / det
            m1, m2 = {}, {}
            for g in range(g0, G):
                p, q = v[c][g], v[c + 1][g]
                if g == g0:
                    if i0 == 6:
                        continue
                    p, q = jnp.where(sub > i0 + 1, p, 0.0), jnp.where(sub > i0 + 1, q, 0.0)
                m1[g] = (p * e - q * b) * inv
                m2[g] = (q * a - p * b) * inv
            for m in range(c + 2, SUB):
                p, q = row_of(v[m][g0], i0), row_of(v[m][g0], i0 + 1)
                for g in m1:
                    v[m][g] = (v[m][g] - m1[g] * p) - m2[g] * q
            ia = 1.0 / a
            second = jnp.where(sub == i0 + 1, b * ia, 0.0)
            for h in range(H):
                p, q = row_of(r[g0][h], i0), row_of(r[g0][h], i0 + 1)
                for g in m1:
                    r[g][h] = (r[g][h] - m1[g] * p) - m2[g] * q
                r[g0][h] = r[g0][h] - second * p
            diag[s + c], diag[s + c + 1] = a, det * ia
    out = []
    for g in range(G):
        d = diag[8 * g]
        for i in range(1, 8):
            d = jnp.where(sub == i, diag[8 * g + i], d)
        scale = lax.rsqrt(d)
        h0, w = o // 128, o % 128
        done = 8 * g // SUB * SUB + SUB
        if done < LEAF:
            r[g][h0] = jnp.where((lane >= w + done) & (lane < w + LEAF), 0.0, r[g][h0])
        out.append(jnp.concatenate([x * scale for x in r[g]], axis=1))
    return jnp.concatenate(out, axis=0)


def factor(a_ref):
    for k in range(PIV // LEAF):
        o = k * LEAF
        u = leaf(a_ref, o)
        lane = lax.broadcasted_iota(jnp.int32, (LEAF, PIV), 1)
        a_ref[pl.ds(o, LEAF), :] = jnp.where(lane < o + LEAF, u, 0.0)
        left = PIV - o - LEAF
        if left:
            h, m, l = split3(u)
            lhs = jnp.concatenate((h, h, m, m, h, l), axis=0)
            rhs = jnp.concatenate((h, m, h, m, l, h), axis=0)
            start = ((o + LEAF) // 128) * 128
            lt = lhs[:, start:].T
            lt = lt[o + LEAF - start:, :]
            upd = dot(lt, rhs)
            lane = lax.broadcasted_iota(jnp.int32, (left, PIV), 1)
            old = a_ref[pl.ds(o + LEAF, left), :]
            old = jnp.where((lane >= o) & (lane < o + LEAF), 0.0, old)
            a_ref[pl.ds(o + LEAF, left), :] = old - upd


def dot_t(a, b):
    return lax.dot_general(a, b, (((1,), (1,)), ((), ())), preferred_element_type=f32)


def dot6(ls, rs, dot=dot):
    lh, lm, ll = ls
    rh, rm, rl = rs
    return (dot(ll, rh) + dot(lh, rl) + dot(lm, rm)) + (dot(lm, rh) + dot(lh, rm)) + dot(lh, rh)


def dot3(ls, rs):
    lh, lm = ls[:2]
    rh, rm = rs[:2]
    return (dot(lm, rh) + dot(lh, rm)) + dot(lh, rh)


def kernel_b(pid_ref, pt_ref, fr_ref, fc_ref, krc_ref, panel_hbm, schur_hbm,
             a_ref, kr_ref, kc_ref, pc_ref, panel_ref, schur_ref, sems, *, tile):
    n_rows, n_cols = krc_ref.shape
    row0 = lax.axis_index("row") * n_rows
    col0 = lax.axis_index("col") * n_cols
    piv = pid_ref[...]
    pt = jnp.concatenate([pt_ref[0], pt_ref[1]], axis=1)
    fp = features(pt, False)
    fpl = features(pt, True).T
    kpp = jnp.exp(dot(fpl, fp))
    i = lax.broadcasted_iota(jnp.int32, (PIV, PIV), 0)
    j = lax.broadcasted_iota(jnp.int32, (PIV, PIV), 1)
    a_ref[...] = jnp.where(i == j, kpp + 0.1, kpp)
    kpc = jnp.exp(dot(fpl, fc_ref[...]))
    ids = jnp.broadcast_to(piv.astype(f32), (8, PIV)).T[:, 0:1].astype(jnp.int32)
    cid = col0 + lax.broadcasted_iota(jnp.int32, (PIV, n_cols), 1)
    kpc = kpc + jnp.where(cid == ids, 0.1, 0.0)
    for q, x in enumerate(split3(kpc)):
        kc_ref[q] = x
    for t in range(0, n_rows, 256):
        krp = jnp.exp(dot(fr_ref[t:t + 256, :], fp))
        rid = row0 + t + lax.broadcasted_iota(jnp.int32, (256, PIV), 0)
        krp = krp + jnp.where(rid == piv, 0.1, 0.0)
        for q, x in enumerate(split3(krp)):
            kr_ref[q, t:t + 256, :] = x

    factor(a_ref)
    ws = split3(a_ref[...])
    pc = dot6(ws, (kc_ref[0], kc_ref[1], kc_ref[2]))
    for q, x in enumerate(split3(pc)):
        pc_ref[q] = x

    copies = []

    def send(src, dst):
        copy = pltpu.make_async_copy(src, dst, sems.at[len(copies)])
        copy.start()
        copies.append(copy)

    half = n_cols // 2
    for t in range(0, n_rows, tile):
        rows = pl.ds(t, tile)
        panel = dot6(tuple(kr_ref[q, t:t + tile, :] for q in range(3)), ws, dot_t)
        panel_ref[rows, :] = panel
        send(panel_ref.at[rows, :], panel_hbm.at[rows, :])
        ps = split3(panel)
        for c in range(0, n_cols, half):
            cols = pl.ds(c, half)
            schur_ref[rows, cols] = krc_ref[rows, cols] - dot6(ps, tuple(pc_ref[q, :, c:c + half] for q in range(3)))
            send(schur_ref.at[rows, cols], schur_hbm.at[rows, cols])
    for copy in copies:
        copy.wait()


def compute(pid, pt, fr, fc, krc, tile=1024):
    n_rows, n_cols = krc.shape
    vmem = pl.BlockSpec(memory_space=pltpu.VMEM)
    hbm = pl.BlockSpec(memory_space=pltpu.HBM)
    return pl.pallas_call(
        functools.partial(kernel_b, tile=tile),
        out_shape=(
            jax.ShapeDtypeStruct((n_rows, PIV), f32),
            jax.ShapeDtypeStruct((n_rows, n_cols), f32),
        ),
        in_specs=[vmem] * 5,
        out_specs=(hbm, hbm),
        scratch_shapes=[
            pltpu.VMEM((PIV, PIV), f32),
            pltpu.VMEM((3, n_rows, PIV), bf16),
            pltpu.VMEM((3, PIV, n_cols), bf16),
            pltpu.VMEM((3, PIV, n_cols), bf16),
            pltpu.VMEM((n_rows, PIV), f32),
            pltpu.VMEM((n_rows, n_cols), f32),
            pltpu.SemaphoreType.DMA((3 * n_rows // tile,)),
        ],
        compiler_params=pltpu.CompilerParams(vmem_limit_bytes=32 << 20),
    )(pid, pt, fr, fc, krc)


MESH = pl.DeviceIdType.MESH
NX = 4


def loop(lo, hi, f):
    def body(i, carry):
        f(i)
        return carry
    lax.fori_loop(lo, hi, body, 0)


def unpack(buf_ref, out_ref):
    k = buf_ref.shape[0]
    tiles = k // 4
    lane = lax.broadcasted_iota(jnp.int32, (4 * tiles, 128), 1) // 32
    quads = []
    for q in range(4):
        quads.append(jnp.concatenate([buf_ref[4 * t + q] for t in range(tiles)], axis=0))
    for g in range(4):
        acc = quads[g]
        for q in range(4):
            if q != g:
                acc = jnp.where(lane == q, pltpu.roll(quads[q], (32 * (q - g)) % 128, 1), acc)
        for t in range(tiles):
            out_ref[4 * g:4 * g + 4, 128 * t:128 * t + 128] = acc[4 * t:4 * t + 4]


def gather_kernel(nz, ny, pts_hbm, pf_hbm, ps_hbm, pid_out, piv_out, fr_out, fc_out, krc_out,
                  pts_ref, in_sem, own, contrib, c_buf, x_src, x_buf, y_src, y_buf, z_src, z_buf,
                  row_buf, col_buf, rt_ref, ct_ref,
                  c_send, c_recv, x_send, x_recv, y_send, y_recv, z_send, z_recv, ag_send, ag_recv,
                  row_send, row_recv, col_send, col_recv):
    n_row, n_col = 2 * nz, ny * NX
    row = lax.axis_index("row")
    col = lax.axis_index("col")
    core, z = row % 2, row // 2
    x, y = col % NX, col // NX
    other = (2 * z + 1 - core, col)

    def x_dev(d):
        return (row, NX * y + (x + d) % NX)

    def y_dev(d):
        return (row, NX * ((y + d) % ny) + x)

    def z_dev(d):
        return (2 * ((z + d) % nz) + core, col)

    def row_dev(d):
        return (row, (col + d) % n_col)

    wide = n_col // n_row
    per = n_col // wide
    target = wide * row + col // per
    part = col % per
    source = col // wide
    first = (col % wide) * per

    arrivals = [
        pltpu.make_async_copy(pts_hbm, pts_ref, in_sem.at[0]),
        pltpu.make_async_copy(pf_hbm, pid_out.at[:, pl.ds(0, BLOCK)], in_sem.at[1]),
        pltpu.make_async_copy(ps_hbm, pid_out.at[:, pl.ds(BLOCK, BLOCK)], in_sem.at[2]),
    ]
    for a in arrivals:
        a.start()
    barrier = pltpu.get_barrier_semaphore()

    def signal(dev):
        pl.semaphore_signal(barrier, inc=1, device_id=dev, device_id_type=MESH)


    def greet_source(i):
        @pl.when(jnp.logical_or(source != row, first + i != col))
        def _():
            signal((source, first + i))

    loop(0, per, greet_source)
    loop(1, nz, lambda d: signal(z_dev(d)))
    loop(1, n_col, lambda d: signal(row_dev(d)))
    signal(other)

    for a in arrivals:
        a.wait()
    pts = pts_ref[...]
    n = pts.shape[1]
    for g in range(4):
        own[:, 32 * g:32 * g + 32] = pts[4 * g:4 * g + 4, :]
    mine = (row * n_col + col) * n
    h, m, l = split3(pts)
    for half in range(2):
        hit = pid_out[:, BLOCK * half:BLOCK * half + BLOCK] == mine + lax.broadcasted_iota(jnp.int32, (n, BLOCK), 0)
        hot = jnp.where(hit, 1.0, 0.0).astype(bf16)
        contrib[half] = (dot(l, hot) + dot(m, hot)) + dot(h, hot)
    row_buf[col] = own[...]

    to_me = n_row - 1 + jnp.where(target == col, 0, 1)
    pl.semaphore_wait(barrier, 1 + (nz - 1) + (n_col - 1) + to_me)

    def remote(src, dst, send, recv, dev):
        return pltpu.make_async_remote_copy(
            src_ref=src, dst_ref=dst, send_sem=send, recv_sem=recv, device_id=dev, device_id_type=MESH)

    def c_copy():
        return remote(contrib.at[1 - core], c_buf, c_send, c_recv, other)

    def x_copy(d):
        return remote(x_src, x_buf.at[d - 1], x_send.at[d - 1], x_recv.at[d - 1], x_dev(d))

    def y_copy(d):
        return remote(y_src, y_buf.at[d - 1], y_send.at[d - 1], y_recv.at[d - 1], y_dev(d))

    def z_copy(d):
        return remote(z_src, z_buf.at[d - 1], z_send.at[d - 1], z_recv.at[d - 1], z_dev(d))

    def ag_copy():
        return remote(piv_out.at[core], piv_out.at[core], ag_send, ag_recv, other)

    def row_copy(d):
        return remote(own, row_buf.at[col], row_send.at[d - 1], row_recv.at[d - 1], row_dev(d))

    def col_copy(d):
        return remote(own, col_buf.at[part], col_send.at[d], col_recv.at[part], ((row + d) % n_row, target))

    def col_arrival(i):
        return remote(own, col_buf.at[i], col_send.at[0], col_recv.at[i], (row, col))

    c_copy().start()
    loop(1, n_col, lambda d: row_copy(d).start())

    @pl.when(target != col)
    def _():
        col_copy(0).start()

    @pl.when(target == col)
    def _():
        col_buf[part] = own[...]

    loop(1, n_row, lambda d: col_copy(d).start())

    c_copy().wait_recv()
    total = contrib[core] + c_buf[...]
    x_src[...] = total
    for d in range(1, NX):
        x_copy(d).start()
    for d in range(1, NX):
        x_copy(d).wait_recv()
        total = total + x_buf[d - 1]
    y_src[...] = total
    for d in range(1, ny):
        y_copy(d).start()
    for d in range(1, ny):
        y_copy(d).wait_recv()
        total = total + y_buf[d - 1]
    z_src[...] = total
    for d in range(1, nz):
        z_copy(d).start()

    loop(1, n_col, lambda d: row_copy(d).wait_recv())

    def take(i):
        @pl.when(jnp.logical_or(source != row, first + i != col))
        def _():
            col_arrival(i).wait_recv()

    loop(0, per, take)
    unpack(row_buf, rt_ref)
    unpack(col_buf, ct_ref)
    fr_out[...] = features(rt_ref[...], True).T
    fc_out[...] = features(ct_ref[...], False)
    n_cols = fc_out.shape[1]
    off = col * n_cols - row * fr_out.shape[0]
    step = 256

    def block(b):
        at = pl.ds(pl.multiple_of(b * step, step), step)
        i = b * step + lax.broadcasted_iota(jnp.int32, (step, n_cols), 0)
        j = off + lax.broadcasted_iota(jnp.int32, (step, n_cols), 1)
        k = jnp.exp(dot(fr_out[at, :], fc_out[...]))
        krc_out[at, :] = k + jnp.where(i == j, 0.1, 0.0)

    loop(0, fr_out.shape[0] // step, block)

    for d in range(1, nz):
        z_copy(d).wait_recv()
        total = total + z_buf[d - 1]
    piv_out[core] = total
    ag_copy().start()
    c_copy().wait_send()
    for d in range(1, NX):
        x_copy(d).wait_send()
    for d in range(1, ny):
        y_copy(d).wait_send()
    for d in range(1, nz):
        z_copy(d).wait_send()
    loop(1, n_col, lambda d: row_copy(d).wait_send())

    @pl.when(target != col)
    def _():
        col_copy(0).wait_send()

    loop(1, n_row, lambda d: col_copy(d).wait_send())
    ag_copy().wait_recv()
    ag_copy().wait_send()


def gather(points, pf, ps, mesh):
    n_row, n_col = mesh.shape["row"], mesh.shape["col"]
    nz = n_row // 2
    ny = n_col // NX
    n = points.shape[1]
    dma = pltpu.SemaphoreType.DMA
    vmem = pl.BlockSpec(memory_space=pltpu.VMEM)
    return pl.pallas_call(
        functools.partial(gather_kernel, nz, ny),
        out_shape=(
            pltpu.VMEM((1, PIV), jnp.int32),
            pltpu.VMEM((2, DIM, BLOCK), f32),
            pltpu.VMEM((n * n_col, 128), bf16),
            pltpu.VMEM((128, n * n_row), bf16),
            pltpu.VMEM((n * n_col, n * n_row), f32),
        ),
        in_specs=[pl.BlockSpec(memory_space=pltpu.HBM)] * 3,
        out_specs=(vmem,) * 5,
        scratch_shapes=[
            pltpu.VMEM((DIM, n), f32),
            dma((3,)),
            pltpu.VMEM((4, 128), f32),
            pltpu.VMEM((2, DIM, BLOCK), f32),
            pltpu.VMEM((DIM, BLOCK), f32),
            pltpu.VMEM((DIM, BLOCK), f32),
            pltpu.VMEM((NX - 1, DIM, BLOCK), f32),
            pltpu.VMEM((DIM, BLOCK), f32),
            pltpu.VMEM((ny - 1, DIM, BLOCK), f32),
            pltpu.VMEM((DIM, BLOCK), f32),
            pltpu.VMEM((nz - 1, DIM, BLOCK), f32),
            pltpu.VMEM((n_col, 4, 128), f32),
            pltpu.VMEM((n_row, 4, 128), f32),
            pltpu.VMEM((DIM, n * n_col), f32),
            pltpu.VMEM((DIM, n * n_row), f32),
            dma, dma,
            dma((NX - 1,)), dma((NX - 1,)),
            dma((ny - 1,)), dma((ny - 1,)),
            dma((nz - 1,)), dma((nz - 1,)),
            dma, dma,
            dma((n_col - 1,)), dma((n_col - 1,)),
            dma((n_row,)), dma((n_row,)),
        ],
        compiler_params=pltpu.CompilerParams(
            collective_id=0, has_side_effects=True, vmem_limit_bytes=8 << 20),
    )(points, pf, ps)


def solution(mesh):
    def per_device(points, pivots_first, pivots_second):
        points, pf, ps = (
            pltpu.with_memory_space_constraint(x, pltpu.HBM)
            for x in (points, pivots_first[None, :], pivots_second[None, :]))
        return compute(*gather(points, pf, ps, mesh))

    return jax.shard_map(
        per_device,
        mesh=mesh,
        in_specs=(P(None, ("row", "col")), P(), P()),
        out_specs=(P("row", None), P("row", "col")),
        check_vma=False,
    )
```
